32 devices in a mesh: grp: 2 (over y), seq: 4 (over z), head: 2 (over x), rep: 2 (over core).
Axes of the slice: x: 2, y: 2, z: 4, core: 2. Of those that a mesh axis runs over, the one named last changes fastest.
Arguments:
- queries: bfloat16 [32, 64, 128], P(('grp', 'rep'), 'head'), parts along dimension 0, may hold values from -16 to 16
- key_cache: bfloat16 [32, 4, 2048, 128], P(('grp', 'rep'), 'head', 'seq'), parts along dimension 0, may hold values from -7 to 7
- value_cache: bfloat16 [32, 4, 2048, 128], P(('grp', 'rep'), 'head', 'seq'), parts along dimension 0, may hold values from -6 to 6
- indices: int32 [32, 4, 16], P(('grp', 'rep'), 'head'), parts along dimension 0, may hold values from 0 to 31, as said below
- counts: int32 [32, 4], P(('grp', 'rep'), 'head'), parts along dimension 0, may hold values from 8 to 16, as said below
- lengths: int32 [32], P(('grp', 'rep')), parts along dimension 0, may hold values from 1024 to 2048
Outputs:
- attended: bfloat16 [32, 64, 128], P(('grp', 'rep'), 'head', 'seq'), parts along dimension 0
The draws below stay inside these ranges and needn't reach their ends.
There are 2 independent parts, one for each index of `grp`. The reference program is written for one: setup_inputs(seed, part) draws one part's arguments, and reference() takes and returns one part's arrays. A program takes and returns all parts, laid end to end along the dimension named above; each array names one. Nothing has to cross between parts.
Inputs may be any that keep to these rules, and one draw needn't show every extreme that they name: `indices`: within a row and key-value head the 16 blocks are distinct, and each holds at least one token below the row's length. `counts`: some row uses all 16 slots.
All inputs are finite; a program needn't handle non-finite values.
Results may differ from the reference program's by a relative error of at most 0.0015.
Values sent between devices are 32-bit elements; how exact they have to be, the bound alone decides.
A program may use at most 64 MiB of HBM per device.

```python
import jax
import jax.numpy as jnp
from jax import lax

HEADS = 64
KVH = 4
DK = 128
DV = 128
BLOCK = 64
SLOTS = 16
BATCH = 16
CONTEXT = 2048


def selection(key):
    lengths = jax.random.randint(jax.random.fold_in(key, 11), (BATCH,), CONTEXT // 2, CONTEXT + 1)
    counts = jax.random.randint(jax.random.fold_in(key, 12), (BATCH, KVH), SLOTS // 2, SLOTS + 1)
    counts = jnp.where(jnp.arange(BATCH)[:, None] == 0, SLOTS, counts)
    blocks = CONTEXT // BLOCK
    finals = (lengths - 1) // BLOCK
    noise = jax.random.randint(jax.random.fold_in(key, 13), (BATCH, KVH, blocks), 0, 1 << 16)
    numbers = jnp.arange(blocks)
    noise = noise * blocks + numbers[None, None, :]
    inside = (numbers[None, None, :] >= 1) & (numbers[None, None, :] < finals[:, None, None])
    ranked = jnp.where(inside, noise, noise + (1 << 16) * blocks)
    order = jnp.argsort(ranked, axis=-1, stable=True)[:, :, :SLOTS - 2]
    first = jnp.zeros((BATCH, KVH, 1), jnp.int32)
    latest = jnp.broadcast_to(finals[:, None, None], (BATCH, KVH, 1))
    indices = jnp.concatenate([first, latest.astype(jnp.int32), order.astype(jnp.int32)], axis=-1)
    return (lengths.astype(jnp.int32), counts.astype(jnp.int32), indices)


def draw_indices(key, part):
    return selection(key)[2]


def draw_counts(key, part):
    return selection(key)[1]


def draw_lengths(key, part):
    return selection(key)[0]


def draw_queries(key, part):
    base = jnp.clip(4.0 * jax.random.normal(jax.random.fold_in(key, 3), (BATCH, HEADS, DK), jnp.float32), -16.0, 16.0)
    return base.astype(jnp.bfloat16)


def draw_key_cache(key, part):
    base = jnp.clip(jax.random.normal(jax.random.fold_in(key, 5), (BATCH, KVH, CONTEXT, DK), jnp.float32), -7.0, 7.0)
    return base.astype(jnp.bfloat16)


def steps_of(own_key, extent, split, smallest, high):
    gain = 1.0
    for dim, shards_of in split:
        heights = jax.random.uniform(jax.random.fold_in(jax.random.fold_in(own_key, 6), dim), (shards_of,), jnp.float32, smallest / len(split), high / len(split))
        gain = gain * jnp.repeat(jnp.exp(heights), extent[dim] // shards_of).reshape((-1,) + (1,) * (len(extent) - 1 - dim))
    return gain


def gaussian(key, dims, width, most, cuts=(), kind=jnp.bfloat16):
    result = width * jax.random.normal(key, dims, jnp.float32)
    if cuts:
        result = result * steps_of(key, dims, cuts, -0.22, 0.18)
    return jnp.clip(result, -most, most).astype(kind)


def setup_inputs(seed: int = 0, part: int = 0) -> dict:
    seeds = jax.random.split(jax.random.key(seed), 7)
    part_keys = jax.random.split(jax.random.fold_in(seeds[6], part), 7)
    return {
        "queries": draw_queries(jax.random.fold_in(jax.random.fold_in(seeds[6], part), 71), part),
        "key_cache": draw_key_cache(jax.random.fold_in(jax.random.fold_in(seeds[6], part), 71), part),
        "value_cache": gaussian(part_keys[2], (BATCH, KVH, CONTEXT, DV), 1.0, 6.0, ((0, 2), (1, 2), (2, 4))),
        "indices": draw_indices(jax.random.fold_in(jax.random.fold_in(seeds[6], part), 71), part),
        "counts": draw_counts(jax.random.fold_in(jax.random.fold_in(seeds[6], part), 71), part),
        "lengths": draw_lengths(jax.random.fold_in(jax.random.fold_in(seeds[6], part), 71), part),
    }


def attend_row(packed):
    query_row, key_row, value_row, index_row, count_row, length_row = packed
    group = HEADS // KVH
    rescale_factor = DK ** -0.5
    query_grouped = query_row.reshape(KVH, group, DK).astype(jnp.float32)
    key_blocks = key_row.reshape(KVH, CONTEXT // BLOCK, BLOCK, DK)
    value_blocks = value_row.reshape(KVH, CONTEXT // BLOCK, BLOCK, DV)
    chosen = index_row.astype(jnp.int32)
    chosen_keys = jnp.take_along_axis(key_blocks, chosen[:, :, None, None], axis=1)
    chosen_keys = chosen_keys.reshape(KVH, SLOTS * BLOCK, DK).astype(jnp.float32)
    picked_value_rows = jnp.take_along_axis(value_blocks, chosen[:, :, None, None], axis=1)
    picked_value_rows = picked_value_rows.reshape(KVH, SLOTS * BLOCK, DV).astype(jnp.float32)
    offsets = jnp.arange(BLOCK, dtype=jnp.int32)
    position = chosen[:, :, None] * BLOCK + offsets[None, None, :]
    used = jnp.arange(SLOTS, dtype=jnp.int32)[None, :, None] < count_row[:, None, None]
    live = (used & (position < length_row)).reshape(KVH, SLOTS * BLOCK)
    scores = jnp.einsum("hgd,hkd->hgk", query_grouped, chosen_keys, precision=lax.Precision.HIGHEST) * rescale_factor
    scores = jnp.where(live[:, None, :], scores, -jnp.inf)
    highest = jnp.max(scores, axis=-1, keepdims=True)
    softmax_weights = jnp.exp(scores - highest)
    total = jnp.sum(softmax_weights, axis=-1)
    weighted_value_sum = jnp.einsum("xcd,xdr->xcr", softmax_weights, picked_value_rows, precision=lax.Precision.HIGHEST)
    return (weighted_value_sum / total[..., None]).reshape(HEADS, DV).astype(jnp.bfloat16)


def reference(queries, key_cache, value_cache, indices, counts, lengths):
    return lax.map(attend_row, (queries, key_cache, value_cache, indices, counts, lengths))
```

```python
import functools

import jax
import jax.numpy as jnp
from jax import lax
from jax.experimental import pallas as pl
from jax.experimental.pallas import tpu as pltpu
from jax.sharding import PartitionSpec as P

BLOCK = 64
LOWEST = -1e30
SUB = 8
LANES = 128


def block_transpose(vregs, share):
    n = len(vregs)
    lane_group = lax.broadcasted_iota(jnp.int32, (SUB, LANES), 1) // share
    step = 1
    while step < n:
        low = (lane_group // step) % 2 == 0
        nxt = list(vregs)
        for g in range(n):
            if (g // step) % 2 == 0:
                a, b = vregs[g], vregs[g + step]
                nxt[g] = jnp.where(low, a, pltpu.roll(b, step * share, 1))
                nxt[g + step] = jnp.where(low, pltpu.roll(a, LANES - step * share, 1), b)
        vregs = nxt
        step *= 2
    return vregs


def kernel(n, rows_per_message, q_hbm, k_hbm, v_hbm, idx_hbm, cnt_hbm, len_hbm, out_ref,
           q_ref, k_ref, v_ref, idx_ref, cnt_ref, len_ref, send_buf, recv_buf,
           in_sem, kv_sem, send_sem, recv_sem):
    batch, heads, ctx, width = k_ref.shape
    group = q_ref.shape[1] // heads
    slots = idx_ref.shape[1]
    share = LANES // n
    groups = batch * heads * group // SUB
    chunks = pl.cdiv(groups, n)
    me = lax.axis_index("seq")

    small = [
        pltpu.make_async_copy(src, dst, in_sem.at[i])
        for i, (src, dst) in enumerate(
            ((idx_hbm, idx_ref), (cnt_hbm, cnt_ref), (len_hbm, len_ref), (q_hbm, q_ref))
        )
    ]
    for copy in small:
        copy.start()
    loads = []
    for b in range(batch):
        k_copy = pltpu.make_async_copy(k_hbm.at[b], k_ref.at[b], kv_sem.at[0, b])
        v_copy = pltpu.make_async_copy(v_hbm.at[b], v_ref.at[b], kv_sem.at[1, b])
        k_copy.start()
        v_copy.start()
        loads.append((k_copy, v_copy))

    barrier = pltpu.get_barrier_semaphore()
    for k in range(1, n):
        pl.semaphore_signal(
            barrier, inc=1, device_id={"seq": lax.rem(me + k, n)},
            device_id_type=pl.DeviceIdType.MESH,
        )

    for copy in small:
        copy.wait()

    pairs = batch * heads
    pair = lax.broadcasted_iota(jnp.int32, (pairs, batch), 0)
    row = lax.broadcasted_iota(jnp.int32, (pairs, batch), 1)
    own = pair // heads == row
    length_rows = jnp.broadcast_to(len_ref[...], (pairs, batch)).astype(jnp.float32)
    length = jnp.sum(jnp.where(own, length_rows, 0.0), axis=1, keepdims=True)
    count = jnp.zeros((pairs, 1), jnp.float32)
    for h in range(heads):
        count_rows = jnp.broadcast_to(cnt_ref[h : h + 1, :], (pairs, batch)).astype(jnp.float32)
        count += jnp.sum(
            jnp.where(own & (pair % heads == h), count_rows, 0.0), axis=1, keepdims=True
        )
    slot = lax.broadcasted_iota(jnp.int32, (pairs, slots), 1)
    chosen = jnp.where(slot < count.astype(jnp.int32), idx_ref[...], -1)
    position = me * ctx + lax.broadcasted_iota(jnp.int32, (pairs, ctx), 1)
    block = position // BLOCK
    picked = chosen[:, 0:1] == block
    for s in range(1, slots):
        picked |= chosen[:, s : s + 1] == block
    live = picked & (position < length.astype(jnp.int32))
    bias = jnp.where(live, 0.0, -jnp.inf)

    scale = width ** (-0.5)
    lane = lax.broadcasted_iota(jnp.int32, (SUB, LANES), 1)
    stats = jnp.zeros((SUB, LANES), jnp.float32)
    pending = []
    sends = []
    done = 0
    sent = 0
    message = 0

    def send(first, last, message):
        for k in sorted(range(1, n), key=lambda k: (abs(k - n // 2), -k)):
            peer = lax.rem(me + k, n)
            copy = pltpu.make_async_remote_copy(
                src_ref=send_buf.at[peer, pl.ds(first, last - first)],
                dst_ref=recv_buf.at[k - 1, pl.ds(first, last - first)],
                send_sem=send_sem.at[k - 1, message],
                recv_sem=recv_sem.at[k - 1, message],
                device_id={"seq": peer},
                device_id_type=pl.DeviceIdType.MESH,
            )
            copy.start()
            sends.append(copy)

    for b in range(batch):
        loads[b][0].wait()
        loads[b][1].wait()
        for h in range(heads):
            p_index = b * heads + h
            q = q_ref[b, h * group : (h + 1) * group, :]
            scores = lax.dot_general(
                q, k_ref[b, h], (((1,), (1,)), ((), ())), preferred_element_type=jnp.float32
            )
            scores = scores * scale + bias[p_index : p_index + 1, :]
            top = jnp.maximum(jnp.max(scores, axis=1, keepdims=True), LOWEST)
            weights = jnp.exp(scores - top)
            total = jnp.sum(weights, axis=1, keepdims=True)
            high = weights.astype(jnp.bfloat16)
            rest = (weights - high.astype(jnp.float32)).astype(jnp.bfloat16)
            both = jnp.concatenate([high, rest], axis=0)
            product = jnp.dot(both, v_ref[b, h], preferred_element_type=jnp.float32)
            summed = product[:group] + product[group:]
            for part in range(group // SUB):
                r = p_index * (group // SUB) + part
                c, g = r // n, r % n
                rows = slice(part * SUB, (part + 1) * SUB)
                stats = jnp.where(lane == g * share + c, top[rows], stats)
                stats = jnp.where(lane == g * share + chunks + c, total[rows], stats)
                pending.append(summed[rows])
                if r == groups - 1:
                    pending += [jnp.zeros((SUB, LANES), jnp.float32)] * (n - len(pending))
                if len(pending) == n:
                    for d, packed in enumerate(block_transpose(pending, share)):
                        send_buf[d, c] = packed
                    pending = []
                    done = c + 1
        if b == batch - 1:
            for d in range(n):
                send_buf[d, chunks] = stats
            done = chunks + 1
        if done - sent >= rows_per_message or (b == batch - 1 and done > sent):
            if sent == 0:
                pl.semaphore_wait(barrier, n - 1)
            send(sent, done, message)
            sent = done
            message += 1

    for copy in sends:
        copy.wait_recv()

    sources = [recv_buf.at[k] for k in range(n - 1)]
    held = [stats] + [source[chunks] for source in sources]
    highest = functools.reduce(jnp.maximum, held)
    factors = [jnp.exp(jnp.minimum(h - highest, 0.0)) for h in held]
    totals = [pltpu.roll(h, LANES - chunks, 1) for h in held]
    total = functools.reduce(jnp.add, [f * t for f, t in zip(factors, totals)])
    is_top = lane % share < chunks
    inverse = 1.0 / jnp.where(is_top, total, 1.0)
    factors = [jnp.where(is_top, f * inverse, 0.0) for f in factors]
    base = lane // share * share
    finished = []
    for c in range(chunks):
        result = None
        for i in range(n):
            factor = jnp.take_along_axis(factors[i], base + c, axis=1)
            data = send_buf[me, c] if i == 0 else sources[i - 1][c]
            term = factor * data
            result = term if result is None else result + term
        for g in range(n):
            moved = result if g == 0 else pltpu.roll(result, LANES - g * share, 1)
            finished.append(moved[:, :share])
    per_row = heads * group // SUB
    for b in range(batch):
        out_ref[b] = jnp.concatenate(
            finished[b * per_row : (b + 1) * per_row], axis=0
        ).astype(out_ref.dtype)

    for copy in sends:
        copy.wait_send()


def solution(mesh):
    n = mesh.shape["seq"]

    def local(queries, key_cache, value_cache, indices, counts, lengths):
        batch, heads, ctx, width = key_cache.shape
        value_width = value_cache.shape[3]
        all_heads = queries.shape[1]
        slots = indices.shape[2]
        chunks = pl.cdiv(batch * all_heads // SUB, n)
        rows_per_message = max(1, chunks // 4)
        messages = chunks // rows_per_message + 1
        return pl.pallas_call(
            functools.partial(kernel, n, rows_per_message),
            out_shape=jax.ShapeDtypeStruct(
                (batch, all_heads, value_width // n), jnp.bfloat16
            ),
            in_specs=[pl.BlockSpec(memory_space=pl.ANY)] * 6,
            out_specs=pl.BlockSpec(memory_space=pltpu.VMEM),
            scratch_shapes=[
                pltpu.VMEM(queries.shape, queries.dtype),
                pltpu.VMEM(key_cache.shape, key_cache.dtype),
                pltpu.VMEM(value_cache.shape, value_cache.dtype),
                pltpu.VMEM((batch * heads, slots), jnp.int32),
                pltpu.VMEM((heads, batch), jnp.int32),
                pltpu.VMEM((1, batch), jnp.int32),
                pltpu.VMEM((n, chunks + 1, SUB, LANES), jnp.float32),
                pltpu.VMEM((n - 1, chunks + 1, SUB, LANES), jnp.float32),
                pltpu.SemaphoreType.DMA((4,)),
                pltpu.SemaphoreType.DMA((2, batch)),
                pltpu.SemaphoreType.DMA((n - 1, messages)),
                pltpu.SemaphoreType.DMA((n - 1, messages)),
            ],
            compiler_params=pltpu.CompilerParams(collective_id=0, has_side_effects=True),
        )(
            queries,
            key_cache,
            value_cache,
            indices.reshape(batch * heads, slots),
            counts.T,
            lengths.reshape(1, batch),
        )

    return jax.shard_map(
        local,
        mesh=mesh,
        in_specs=(
            P(("grp", "rep"), "head", None),
            P(("grp", "rep"), "head", "seq", None),
            P(("grp", "rep"), "head", "seq", None),
            P(("grp", "rep"), "head", None),
            P(("grp", "rep"), "head"),
            P(("grp", "rep")),
        ),
        out_specs=P(("grp", "rep"), "head", "seq"),
        check_vma=False,
    )
```

```python
import functools

import jax
import jax.numpy as jnp
from jax import lax
from jax.experimental import pallas as pl
from jax.experimental.pallas import tpu as pltpu
from jax.sharding import PartitionSpec as P

BLOCK = 64
LOWEST = -1e30
SUB = 8
RUN = 4
LOAD_RUN = 4
MESSAGES = 2
LANES = 128


def block_transpose(vregs, share):
    n = len(vregs)
    lane_group = lax.broadcasted_iota(jnp.int32, (SUB, LANES), 1) // share
    step = 1
    while step < n:
        low = (lane_group // step) % 2 == 0
        nxt = list(vregs)
        for g in range(n):
            if (g // step) % 2 == 0:
                a, b = vregs[g], vregs[g + step]
                nxt[g] = jnp.where(low, a, pltpu.roll(b, step * share, 1))
                nxt[g + step] = jnp.where(low, pltpu.roll(a, LANES - step * share, 1), b)
        vregs = nxt
        step *= 2
    return vregs


def kernel(n, rows_per_message, run, load_run, q_hbm, k_hbm, v_hbm, idx_hbm, cnt_hbm, len_hbm, out_ref,
           q_ref, k_ref, v_ref, idx_ref, cnt_ref, len_ref, score_ref, weight_ref,
           send_buf, recv_buf,
           in_sem, kv_sem, send_sem, recv_sem):
    batch, heads, ctx, width = k_ref.shape
    group = q_ref.shape[1] // heads
    slots = idx_ref.shape[1]
    share = LANES // n
    groups = batch * heads * group // SUB
    chunks = pl.cdiv(groups, n)
    me = lax.axis_index("seq")

    barrier = pltpu.get_barrier_semaphore()
    for k in range(1, n):
        pl.semaphore_signal(
            barrier, inc=1, device_id={"seq": lax.rem(me + k, n)},
            device_id_type=pl.DeviceIdType.MESH,
        )

    small = [
        pltpu.make_async_copy(src, dst, in_sem.at[i])
        for i, (src, dst) in enumerate(
            ((idx_hbm, idx_ref), (cnt_hbm, cnt_ref), (len_hbm, len_ref), (q_hbm, q_ref))
        )
    ]
    for copy in small:
        copy.start()
    loads = [
        [
            pltpu.make_async_copy(src.at[b], dst.at[b], kv_sem.at[i, b])
            for i, (src, dst) in enumerate(((k_hbm, k_ref), (v_hbm, v_ref)))
        ]
        for b in range(batch)
    ]
    for i in range(2):
        for load in loads:
            load[i].start()

    for copy in small:
        copy.wait()

    pairs = batch * heads
    pair = lax.broadcasted_iota(jnp.int32, (pairs, batch), 0)
    row = lax.broadcasted_iota(jnp.int32, (pairs, batch), 1)
    own = pair // heads == row
    length_rows = jnp.broadcast_to(len_ref[...], (pairs, batch)).astype(jnp.float32)
    length = jnp.sum(jnp.where(own, length_rows, 0.0), axis=1, keepdims=True)
    count = jnp.zeros((pairs, 1), jnp.float32)
    for h in range(heads):
        count_rows = jnp.broadcast_to(cnt_ref[h : h + 1, :], (pairs, batch)).astype(jnp.float32)
        count += jnp.sum(
            jnp.where(own & (pair % heads == h), count_rows, 0.0), axis=1, keepdims=True
        )
    slot = lax.broadcasted_iota(jnp.int32, (pairs, slots), 1)
    chosen = jnp.where(slot < count.astype(jnp.int32), idx_ref[...], -1)
    position = me * ctx + lax.broadcasted_iota(jnp.int32, (pairs, ctx), 1)
    block = position // BLOCK
    picked = chosen[:, 0:1] == block
    for s in range(1, slots):
        picked |= chosen[:, s : s + 1] == block
    live = picked & (position < length.astype(jnp.int32))
    bias = jnp.where(live, 0.0, -jnp.inf)

    scale = width ** (-0.5)
    lane = lax.broadcasted_iota(jnp.int32, (SUB, LANES), 1)
    stats = jnp.zeros((SUB, LANES), jnp.float32)
    pending = []
    sends = []
    done = 0
    sent = 0
    message = 0

    def send(first, last, message):
        for k in sorted(range(1, n), key=lambda k: (abs(k - n // 2), -k)):
            peer = lax.rem(me + k, n)
            copy = pltpu.make_async_remote_copy(
                src_ref=send_buf.at[peer, pl.ds(first, last - first)],
                dst_ref=recv_buf.at[k - 1, pl.ds(first, last - first)],
                send_sem=send_sem.at[k - 1, message],
                recv_sem=recv_sem.at[k - 1, message],
                device_id={"seq": peer},
                device_id_type=pl.DeviceIdType.MESH,
            )
            copy.start()
            sends.append(copy)

    def score(b):
        for h in range(heads):
            scores = lax.dot_general(
                q_ref[b, h * group : (h + 1) * group, :], k_ref[b, h],
                (((1,), (1,)), ((), ())), preferred_element_type=jnp.float32,
            )
            score_ref[b * heads + h] = scores

    def weigh(b, stats):
        for h in range(heads):
            p_index = b * heads + h
            scores = score_ref[p_index] * scale + bias[p_index : p_index + 1, :]
            top = jnp.maximum(jnp.max(scores, axis=1, keepdims=True), LOWEST)
            weights = jnp.exp(scores - top)
            total = jnp.sum(weights, axis=1, keepdims=True)
            high = weights.astype(jnp.bfloat16)
            rest = (weights - high.astype(jnp.float32)).astype(jnp.bfloat16)
            weight_ref[p_index, :group] = high
            weight_ref[p_index, group:] = rest
            for part in range(group // SUB):
                r = p_index * (group // SUB) + part
                c, g = r // n, r % n
                rows = slice(part * SUB, (part + 1) * SUB)
                stats = jnp.where(lane == g * share + c, top[rows], stats)
                stats = jnp.where(lane == g * share + chunks + c, total[rows], stats)
        return stats

    runs = [range(b, min(b + run, batch)) for b in range(0, batch, run)]
    for i in range(len(runs) + 1):
        if i < len(runs):
            for b in runs[i]:
                loads[b][0].wait()
            for b in runs[i]:
                score(b)
        if i > 0:
            for b in runs[i - 1]:
                stats = weigh(b, stats)
    for d in range(n):
        send_buf[d, chunks] = stats

    for b in range(batch):
        if b % load_run == 0:
            for later in range(b, min(b + load_run, batch)):
                loads[later][1].wait()
        for h in range(heads):
            p_index = b * heads + h
            product = jnp.dot(
                weight_ref[p_index], v_ref[b, h], preferred_element_type=jnp.float32
            )
            summed = product[:group] + product[group:]
            for part in range(group // SUB):
                r = p_index * (group // SUB) + part
                c, g = r // n, r % n
                pending.append(summed[part * SUB : (part + 1) * SUB])
                if r == groups - 1:
                    pending += [jnp.zeros((SUB, LANES), jnp.float32)] * (n - len(pending))
                if len(pending) == n:
                    for d, packed in enumerate(block_transpose(pending, share)):
                        send_buf[d, c] = packed
                    pending = []
                    done = c + 1
        if b == batch - 1:
            done = chunks + 1
        if done - sent >= rows_per_message or (b == batch - 1 and done > sent):
            if sent == 0:
                pl.semaphore_wait(barrier, n - 1)
            send(sent, done, message)
            sent = done
            message += 1

    for copy in sends:
        copy.wait_recv()

    sources = [recv_buf.at[k] for k in range(n - 1)]
    held = [stats] + [source[chunks] for source in sources]
    highest = functools.reduce(jnp.maximum, held)
    factors = [jnp.exp(jnp.minimum(h - highest, 0.0)) for h in held]
    totals = [pltpu.roll(h, LANES - chunks, 1) for h in held]
    total = functools.reduce(jnp.add, [f * t for f, t in zip(factors, totals)])
    is_top = lane % share < chunks
    inverse = 1.0 / jnp.where(is_top, total, 1.0)
    factors = [jnp.where(is_top, f * inverse, 0.0) for f in factors]
    base = lane // share * share
    finished = []
    for c in range(chunks):
        result = None
        for i in range(n):
            factor = jnp.take_along_axis(factors[i], base + c, axis=1)
            data = send_buf[me, c] if i == 0 else sources[i - 1][c]
            term = factor * data
            result = term if result is None else result + term
        for g in range(n):
            moved = result if g == 0 else pltpu.roll(result, LANES - g * share, 1)
            finished.append(moved[:, :share])
    per_row = heads * group // SUB
    for b in range(batch):
        out_ref[b] = jnp.concatenate(
            finished[b * per_row : (b + 1) * per_row], axis=0
        ).astype(out_ref.dtype)

    for copy in sends:
        copy.wait_send()


def solution(mesh):
    n = mesh.shape["seq"]

    def local(queries, key_cache, value_cache, indices, counts, lengths):
        batch, heads, ctx, width = key_cache.shape
        value_width = value_cache.shape[3]
        all_heads = queries.shape[1]
        slots = indices.shape[2]
        chunks = pl.cdiv(batch * all_heads // SUB, n)
        rows_per_message = -(-(chunks + 1) // MESSAGES) if MESSAGES == 1 else max(1, chunks // MESSAGES)
        messages = chunks // rows_per_message + 1
        return pl.pallas_call(
            functools.partial(kernel, n, rows_per_message, RUN, LOAD_RUN),
            out_shape=jax.ShapeDtypeStruct(
                (batch, all_heads, value_width // n), jnp.bfloat16
            ),
            in_specs=[pl.BlockSpec(memory_space=pl.ANY)] * 6,
            out_specs=pl.BlockSpec(memory_space=pltpu.VMEM),
            scratch_shapes=[
                pltpu.VMEM(queries.shape, queries.dtype),
                pltpu.VMEM(key_cache.shape, key_cache.dtype),
                pltpu.VMEM(value_cache.shape, value_cache.dtype),
                pltpu.VMEM((batch * heads, slots), jnp.int32),
                pltpu.VMEM((heads, batch), jnp.int32),
                pltpu.VMEM((1, batch), jnp.int32),
                pltpu.VMEM((batch * heads, all_heads // heads, ctx), jnp.float32),
                pltpu.VMEM((batch * heads, 2 * all_heads // heads, ctx), jnp.bfloat16),
                pltpu.VMEM((n, chunks + 1, SUB, LANES), jnp.float32),
                pltpu.VMEM((n - 1, chunks + 1, SUB, LANES), jnp.float32),
                pltpu.SemaphoreType.DMA((4,)),
                pltpu.SemaphoreType.DMA((2, batch)),
                pltpu.SemaphoreType.DMA((n - 1, messages)),
                pltpu.SemaphoreType.DMA((n - 1, messages)),
            ],
            compiler_params=pltpu.CompilerParams(collective_id=0, has_side_effects=True, vmem_limit_bytes=16 << 20),
        )(
            *[
                pltpu.with_memory_space_constraint(x, pltpu.HBM)
                for x in (
                    queries,
                    key_cache,
                    value_cache,
                    indices.reshape(batch * heads, slots),
                    counts.T,
                    lengths.reshape(1, batch),
                )
            ]
        )

    return jax.shard_map(
        local,
        mesh=mesh,
        in_specs=(
            P(("grp", "rep"), "head", None),
            P(("grp", "rep"), "head", "seq", None),
            P(("grp", "rep"), "head", "seq", None),
            P(("grp", "rep"), "head", None),
            P(("grp", "rep"), "head"),
            P(("grp", "rep")),
        ),
        out_specs=P(("grp", "rep"), "head", "seq"),
        check_vma=False,
    )
```

```python
import functools

import jax
import jax.numpy as jnp
from jax import lax
from jax.experimental import pallas as pl
from jax.experimental.pallas import tpu as pltpu
from jax.sharding import PartitionSpec as P

BLOCK = 64
LOWEST = -1e30
SUB = 8
RUN = 4
LOAD_RUN = 4
MESSAGES = 1
LANES = 128


def block_transpose(vregs, share):
    n = len(vregs)
    lane_group = lax.broadcasted_iota(jnp.int32, (SUB, LANES), 1) // share
    step = 1
    while step < n:
        low = (lane_group // step) % 2 == 0
        nxt = list(vregs)
        for g in range(n):
            if (g // step) % 2 == 0:
                a, b = vregs[g], vregs[g + step]
                nxt[g] = jnp.where(low, a, pltpu.roll(b, step * share, 1))
                nxt[g + step] = jnp.where(low, pltpu.roll(a, LANES - step * share, 1), b)
        vregs = nxt
        step *= 2
    return vregs


def kernel(n, rows_per_message, run, load_run, q_hbm, k_hbm, v_hbm, idx_hbm, cnt_hbm, len_hbm, out_ref,
           q_ref, k_ref, v_ref, idx_ref, cnt_ref, len_ref, score_ref, weight_ref,
           send_buf, recv_buf,
           in_sem, kv_sem, send_sem, recv_sem):
    batch, heads, ctx, width = k_ref.shape
    group = q_ref.shape[1] // heads
    slots = idx_ref.shape[1]
    share = LANES // n
    groups = batch * heads * group // SUB
    chunks = pl.cdiv(groups, n)
    me = lax.axis_index("seq")

    barrier = pltpu.get_barrier_semaphore()
    for k in range(1, n):
        pl.semaphore_signal(
            barrier, inc=1, device_id={"seq": lax.rem(me + k, n)},
            device_id_type=pl.DeviceIdType.MESH,
        )

    small = [
        pltpu.make_async_copy(src, dst, in_sem.at[i])
        for i, (src, dst) in enumerate(
            ((idx_hbm, idx_ref), (cnt_hbm, cnt_ref), (len_hbm, len_ref), (q_hbm, q_ref))
        )
    ]
    for copy in small:
        copy.start()
    loads = [
        [
            pltpu.make_async_copy(src.at[b], dst.at[b], kv_sem.at[i, b])
            for i, (src, dst) in enumerate(((k_hbm, k_ref), (v_hbm, v_ref)))
        ]
        for b in range(batch)
    ]
    for i in range(2):
        for load in loads:
            load[i].start()

    for copy in small:
        copy.wait()

    pairs = batch * heads
    pair = lax.broadcasted_iota(jnp.int32, (pairs, batch), 0)
    row = lax.broadcasted_iota(jnp.int32, (pairs, batch), 1)
    own = pair // heads == row
    length_rows = jnp.broadcast_to(len_ref[...], (pairs, batch)).astype(jnp.float32)
    length = jnp.sum(jnp.where(own, length_rows, 0.0), axis=1, keepdims=True)
    count = jnp.zeros((pairs, 1), jnp.float32)
    for h in range(heads):
        count_rows = jnp.broadcast_to(cnt_ref[h : h + 1, :], (pairs, batch)).astype(jnp.float32)
        count += jnp.sum(
            jnp.where(own & (pair % heads == h), count_rows, 0.0), axis=1, keepdims=True
        )
    slot = lax.broadcasted_iota(jnp.int32, (pairs, slots), 1)
    chosen = jnp.where(slot < count.astype(jnp.int32), idx_ref[...], -1)
    position = me * ctx + lax.broadcasted_iota(jnp.int32, (pairs, ctx), 1)
    block = position // BLOCK
    picked = chosen[:, 0:1] == block
    for s in range(1, slots):
        picked |= chosen[:, s : s + 1] == block
    live = picked & (position < length.astype(jnp.int32))
    bias = jnp.where(live, 0.0, -jnp.inf)

    scale = width ** (-0.5)
    lane = lax.broadcasted_iota(jnp.int32, (SUB, LANES), 1)
    stats = jnp.zeros((SUB, LANES), jnp.float32)
    pending = []
    sends = []
    parts = []
    done = 0
    sent = 0
    message = 0

    def exchange(first, last, message, source, peer):
        return pltpu.make_async_remote_copy(
            src_ref=send_buf.at[peer, pl.ds(first, last - first)],
            dst_ref=recv_buf.at[source, pl.ds(first, last - first)],
            send_sem=send_sem.at[peer, message],
            recv_sem=recv_sem.at[source, message],
            device_id={"seq": peer},
            device_id_type=pl.DeviceIdType.MESH,
        )

    upper = 2 * me // n
    peers = []
    for k in range(n - 1):
        down = n - 1 - k
        down = down - 1 + (down - me + n - 1) // n
        up = k + 1 - (me - k + n - 1) // n
        peers.append(upper * up + (1 - upper) * down)
    others = [lax.rem(me + k, n) for k in range(1, n)]

    def send(first, last, message):
        for peer in peers:
            copy = exchange(first, last, message, me, peer)
            copy.start()
            sends.append(copy)
        parts.append((first, last, message))

    def score(b):
        for h in range(heads):
            scores = lax.dot_general(
                q_ref[b, h * group : (h + 1) * group, :], k_ref[b, h],
                (((1,), (1,)), ((), ())), preferred_element_type=jnp.float32,
            )
            score_ref[b * heads + h] = scores

    def weigh(b, stats):
        for h in range(heads):
            p_index = b * heads + h
            scores = score_ref[p_index] * scale + bias[p_index : p_index + 1, :]
            top = jnp.maximum(jnp.max(scores, axis=1, keepdims=True), LOWEST)
            weights = jnp.exp(scores - top)
            total = jnp.sum(weights, axis=1, keepdims=True)
            high = weights.astype(jnp.bfloat16)
            rest = (weights - high.astype(jnp.float32)).astype(jnp.bfloat16)
            weight_ref[p_index, :group] = high
            weight_ref[p_index, group:] = rest
            for part in range(group // SUB):
                r = p_index * (group // SUB) + part
                c, g = r // n, r % n
                rows = slice(part * SUB, (part + 1) * SUB)
                stats = jnp.where(lane == g * share + c, top[rows], stats)
                stats = jnp.where(lane == g * share + chunks + c, total[rows], stats)
        return stats

    runs = [range(b, min(b + run, batch)) for b in range(0, batch, run)]
    for i in range(len(runs) + 1):
        if i < len(runs):
            for b in runs[i]:
                loads[b][0].wait()
            for b in runs[i]:
                score(b)
        if i > 0:
            for b in runs[i - 1]:
                stats = weigh(b, stats)
    for d in range(n):
        send_buf[d, 0] = stats

    for b in range(batch):
        if b % load_run == 0:
            for later in range(b, min(b + load_run, batch)):
                loads[later][1].wait()
        for h in range(heads):
            p_index = b * heads + h
            product = jnp.dot(
                weight_ref[p_index], v_ref[b, h], preferred_element_type=jnp.float32
            )
            summed = product[:group] + product[group:]
            for part in range(group // SUB):
                r = p_index * (group // SUB) + part
                c, g = r // n, r % n
                pending.append(summed[part * SUB : (part + 1) * SUB])
                if r == groups - 1:
                    pending += [jnp.zeros((SUB, LANES), jnp.float32)] * (n - len(pending))
                if len(pending) == n:
                    for d, packed in enumerate(block_transpose(pending, share)):
                        send_buf[d, c + 1] = packed
                    pending = []
                    done = c + 2
        if done - sent >= rows_per_message or (b == batch - 1 and done > sent):
            if sent == 0:
                pl.semaphore_wait(barrier, n - 1)
            send(sent, done, message)
            sent = done
            message += 1

    base = lane // share * share
    is_top = lane % share < chunks
    finished = []
    factors = None
    for first, last, message in parts:
        for source in others:
            exchange(first, last, message, source, me).wait_recv()
        if factors is None:
            held = [stats] + [recv_buf[source, 0] for source in others]
            highest = functools.reduce(jnp.maximum, held)
            factors = [jnp.exp(jnp.minimum(h - highest, 0.0)) for h in held]
            totals = [pltpu.roll(h, LANES - chunks, 1) for h in held]
            total = functools.reduce(jnp.add, [f * t for f, t in zip(factors, totals)])
            inverse = 1.0 / jnp.where(is_top, total, 1.0)
            factors = [jnp.where(is_top, f * inverse, 0.0) for f in factors]
            factors = [
                [jnp.take_along_axis(f, base + c, axis=1) for f in factors]
                for c in range(chunks)
            ]
        for c in range(max(first, 1) - 1, last - 1):
            result = factors[c][0] * send_buf[me, c + 1]
            for i, source in enumerate(others):
                result += factors[c][i + 1] * recv_buf[source, c + 1]
            for g in range(n):
                moved = result if g == 0 else pltpu.roll(result, LANES - g * share, 1)
                finished.append(moved[:, :share])
    per_row = heads * group // SUB
    for b in range(batch):
        out_ref[b] = jnp.concatenate(
            finished[b * per_row : (b + 1) * per_row], axis=0
        ).astype(out_ref.dtype)

    for copy in sends:
        copy.wait_send()


def solution(mesh):
    n = mesh.shape["seq"]

    def local(queries, key_cache, value_cache, indices, counts, lengths):
        batch, heads, ctx, width = key_cache.shape
        value_width = value_cache.shape[3]
        all_heads = queries.shape[1]
        slots = indices.shape[2]
        chunks = pl.cdiv(batch * all_heads // SUB, n)
        rows_per_message = -(-(chunks + 1) // MESSAGES) if MESSAGES == 1 else max(1, chunks // MESSAGES)
        messages = chunks // rows_per_message + 1
        return pl.pallas_call(
            functools.partial(kernel, n, rows_per_message, RUN, LOAD_RUN),
            out_shape=jax.ShapeDtypeStruct(
                (batch, all_heads, value_width // n), jnp.bfloat16
            ),
            in_specs=[pl.BlockSpec(memory_space=pl.ANY)] * 6,
            out_specs=pl.BlockSpec(memory_space=pltpu.VMEM),
            scratch_shapes=[
                pltpu.VMEM(queries.shape, queries.dtype),
                pltpu.VMEM(key_cache.shape, key_cache.dtype),
                pltpu.VMEM(value_cache.shape, value_cache.dtype),
                pltpu.VMEM((batch * heads, slots), jnp.int32),
                pltpu.VMEM((heads, batch), jnp.int32),
                pltpu.VMEM((1, batch), jnp.int32),
                pltpu.VMEM((batch * heads, all_heads // heads, ctx), jnp.float32),
                pltpu.VMEM((batch * heads, 2 * all_heads // heads, ctx), jnp.bfloat16),
                pltpu.VMEM((n, chunks + 1, SUB, LANES), jnp.float32),
                pltpu.VMEM((n, chunks + 1, SUB, LANES), jnp.float32),
                pltpu.SemaphoreType.DMA((4,)),
                pltpu.SemaphoreType.DMA((2, batch)),
                pltpu.SemaphoreType.DMA((n, messages)),
                pltpu.SemaphoreType.DMA((n, messages)),
            ],
            compiler_params=pltpu.CompilerParams(collective_id=0, has_side_effects=True, vmem_limit_bytes=16 << 20),
        )(
            *[
                pltpu.with_memory_space_constraint(x, pltpu.HBM)
                for x in (
                    queries,
                    key_cache,
                    value_cache,
                    indices.reshape(batch * heads, slots),
                    counts.T,
                    lengths.reshape(1, batch),
                )
            ]
        )

    return jax.shard_map(
        local,
        mesh=mesh,
        in_specs=(
            P(("grp", "rep"), "head", None),
            P(("grp", "rep"), "head", "seq", None),
            P(("grp", "rep"), "head", "seq", None),
            P(("grp", "rep"), "head", None),
            P(("grp", "rep"), "head"),
            P(("grp", "rep")),
        ),
        out_specs=P(("grp", "rep"), "head", "seq"),
        check_vma=False,
    )
```
